256 devices in a mesh: tm: 4 (over x), chan: 64 (over z, y, core).
Axes of the slice: x: 4, y: 4, z: 8, core: 2. Of those that a mesh axis runs over, the one named last changes fastest.
Arguments:
- observations: float32 [128, 64, 16384], P('chan', None, 'tm'), may hold values from -6 to 6
- transition: float32 [128, 128, 128], P('chan'), may hold values from -1 to 1, as said below
- obs_map: float32 [128, 64, 128], P('chan'), may hold values from -0.25 to 0.25
- measured_weighting: float32 [128, 64], P('chan'), may hold values from 0.05 to 0.5
- obs_precision: float32 [128, 64], P('chan'), may hold values from 0.3 to 9
- fading: float32 [128, 16384], P('chan', 'tm'), may hold values from 0.5 to 1
Outputs:
- states: float32 [128, 128, 16384], P('chan', None, 'tm')
- batch_nis: float32 [128], P('tm')
The draws below stay inside these ranges and needn't reach their ends.
Inputs may be any that keep to these rules, and one draw needn't show every extreme that they name: Each channel's transition is symmetric with all eigenvalues of magnitude below one.
All inputs are finite; a program needn't handle non-finite values.
Results may differ from the reference program's by a relative error of at most 0.0003.
Values sent between devices are 32-bit elements; how exact they have to be, the bound alone decides.
No kernel may reach another device: no remote copies, remote signals or barrier semaphores. Data moves between devices by JAX's collectives and lax.ppermute only.
A program may use at most 64 MiB of HBM per device.

```python
import math
import jax
import jax.numpy as jnp
from jax import lax

STATE = 128
OBS = 64
MB_FRAMES = 128
PROBE_COUNT = 128
TIMESTEP_COUNT = 16384
MICRO_BATCHES = 128


def draw_transition(key, part):
    first, latter_portion, third = jax.random.split(key, 3)
    upper = math.log(0.05)
    rates = jnp.exp(jax.random.uniform(first, (PROBE_COUNT, STATE), jnp.float32, math.log(0.0001), upper))
    signs = jnp.where(jax.random.randint(latter_portion, (PROBE_COUNT, STATE), 0, 2) == 0, -1.0, 1.0)
    eigen = signs * jnp.exp(-rates)
    basis, unused = jnp.linalg.qr(jax.random.normal(third, (PROBE_COUNT, STATE, STATE), jnp.float32))
    return jnp.einsum('cst,ct,cut->csu', basis, eigen, basis).astype(jnp.float32)


def draw_obs_precision(key, part):
    ramp = 1.0 + 2.0 * jnp.arange(PROBE_COUNT, dtype=jnp.float32) / max(PROBE_COUNT - 1, 1)
    spread = jax.random.uniform(key, (PROBE_COUNT, OBS), jnp.float32, 0.5, 1.5)
    return (spread * ramp[:, None]).astype(jnp.float32)


def draw_fading(key, part):
    first, latter_portion, third = jax.random.split(key, 3)
    lower = 0.9995
    standard_branch = jax.random.uniform(first, (PROBE_COUNT, TIMESTEP_COUNT), jnp.float32, lower, 1.0)
    clustered_blocks = jax.random.bernoulli(latter_portion, 3.0 / TIMESTEP_COUNT, (PROBE_COUNT, TIMESTEP_COUNT))
    discarded_entries = jax.random.uniform(third, (PROBE_COUNT, TIMESTEP_COUNT), jnp.float32, 0.5, 0.8)
    return jnp.where(clustered_blocks, discarded_entries, standard_branch).astype(jnp.float32)


def levels(key, shape, pieces, least, largest):
    level, own = 1.0, jax.random.fold_in(key, 6)
    for position, parts in pieces:
        draws = jnp.exp(jax.random.uniform(jax.random.fold_in(own, position), (parts,), jnp.float32, least / len(pieces), largest / len(pieces)))
        level = level * jnp.repeat(draws, shape[position] // parts).reshape([-1 if axis == position else 1 for axis in range(len(shape))])
    return level


def bell_draw(rng, dims, scale, most, cuts=(), kind=jnp.bfloat16):
    values = jax.random.normal(rng, dims, jnp.float32) * scale
    if len(cuts) > 0:
        values = levels(rng, dims, cuts, -0.22, 0.18) * values
    return jnp.clip(values, min=-most, max=most).astype(kind)


def setup_inputs(seed: int = 0) -> dict:
    splits = jax.random.split(jax.random.key(seed), 7)
    return {
        "observations": bell_draw(splits[0], (PROBE_COUNT, OBS, TIMESTEP_COUNT), 1.0, 6.0, ((0, 64), (2, 4)), jnp.float32),
        "transition": draw_transition(jax.random.fold_in(splits[6], 71), 0),
        "obs_map": bell_draw(splits[2], (PROBE_COUNT, OBS, STATE), (4 * STATE) ** -0.5, 0.25, ((0, 64),), jnp.float32),
        "measured_weighting": jnp.clip(jnp.exp(math.log(0.5) - 2.3025851 * jax.random.uniform(splits[3], (PROBE_COUNT, OBS), jnp.float32) ** levels(splits[3], (PROBE_COUNT, OBS), ((0, 64),), -0.2, 0.2)), 0.05, 0.5),
        "obs_precision": draw_obs_precision(jax.random.fold_in(splits[6], 71), 0),
        "fading": draw_fading(jax.random.fold_in(splits[6], 71), 0),
    }


def filter_block(argument_list):
    transition, obs_map, measured_weighting, obs_precision, observations, fading = argument_list
    highest = lax.Precision.HIGHEST
    gain = jnp.swapaxes(obs_map, 1, 2) * measured_weighting[:, None, :]

    def advance(carried, inputs):
        frame_obs, frame_fading = inputs
        predicted = frame_fading[:, None] * jnp.einsum('bst,bt->bs', transition, carried, precision=highest)
        innovation = frame_obs - jnp.einsum('bos,bs->bo', obs_map, predicted, precision=highest)
        updated = predicted + jnp.einsum('bso,bo->bs', gain, innovation, precision=highest)
        frame_nis = jnp.sum(obs_precision * innovation * innovation)
        return (updated, (updated, frame_nis))
    initial = jnp.zeros((transition.shape[0], transition.shape[1]), jnp.float32)
    inputs = (jnp.moveaxis(observations, 2, 0), jnp.transpose(fading))
    unused, (history, frame_norms) = lax.scan(advance, initial, inputs)
    return (jnp.moveaxis(history, 0, 2), frame_norms)

def reference(observations, transition, obs_map, measured_weighting, obs_precision, fading):
    block_size = math.gcd(PROBE_COUNT, 64)
    blocks = PROBE_COUNT // block_size

    def split_blocks(array):
        return array.reshape((blocks, block_size) + array.shape[1:])
    argument_list = (split_blocks(transition), split_blocks(obs_map), split_blocks(measured_weighting), split_blocks(obs_precision), split_blocks(observations), split_blocks(fading))
    history, frame_norms = lax.map(filter_block, argument_list)
    states = history.reshape(PROBE_COUNT, STATE, TIMESTEP_COUNT)
    totals = jnp.sum(frame_norms, axis=0)
    batch_nis = jnp.sum(totals.reshape(MICRO_BATCHES, MB_FRAMES), axis=1) / (PROBE_COUNT * MB_FRAMES * OBS)
    return (states, batch_nis)
```

```python
import jax
import jax.numpy as jnp
from jax import lax
from jax.experimental import pallas as pl
from jax.experimental.pallas import tpu as pltpu
from jax.sharding import PartitionSpec as P

LANES = 128
CHUNK = 16
PITCH = 17
BATCH = 128
F32 = jnp.float32
BF16 = jnp.bfloat16
HIGHEST = lax.Precision.HIGHEST


def dot(a, b):
    return jnp.dot(a, b, preferred_element_type=F32)


def exact_dot(a, b):
    return jnp.dot(a, b, preferred_element_type=F32, precision=HIGHEST)


def halves(x):
    high = x.astype(BF16)
    low = (x - high.astype(F32)).astype(BF16)
    return high, low


def packed(m):
    high, low = halves(m)
    return jnp.concatenate([high, low], axis=1)


def side_by_side(x):
    high, low = halves(x)
    return jnp.concatenate([high, low], axis=1)


def thirds(x):
    first = x.astype(BF16)
    rest = x - first.astype(F32)
    second = rest.astype(BF16)
    return first, second, (rest - second.astype(F32)).astype(BF16)


def squared(x):
    a, b, c = thirds(x)
    pair = jnp.concatenate([a, b], axis=1)
    out = dot(pair, jnp.concatenate([pair, pair], axis=0))
    rest = dot(jnp.concatenate([a, c], axis=1), jnp.concatenate([c, a], axis=0))
    return out[:, :LANES] + (out[:, LANES:] + rest)


def times(x, both):
    weights = jnp.concatenate([both, both], axis=0)
    out = dot(side_by_side(x), weights)
    width = out.shape[1] // 2
    return out[:, :width] + out[:, width:]


def before(
    y_hbm, f_hbm, t_hbm, h_hbm, w_hbm,
    ends_ref, sums_ref, phi_ref, pairs_ref, fade_ref, powers_ref, last_ref, closed_ref, double_ref,
    gain_ref, seen_ref,
    yt_ref, inv_ref, tree_ref, treef_ref, y_ref, f_ref, t_ref, h_ref, w_ref, in_sem,
):
    small = [
        pltpu.make_async_copy(source, target, in_sem.at[k])
        for k, (source, target) in enumerate(
            ((f_hbm, f_ref), (t_hbm, t_ref), (h_hbm, h_ref), (w_hbm, w_ref))
        )
    ]
    large = pltpu.make_async_copy(y_hbm, y_ref, in_sem.at[4])
    for copy in small:
        copy.start()
    large.start()
    for copy in small:
        copy.wait()
    frames = y_ref.shape[1]
    blocks = frames // LANES
    chunks = frames // CHUNK
    per_block = LANES // CHUNK
    obs = h_ref.shape[1]
    lane = lax.broadcasted_iota(jnp.int32, (1, LANES), 1)

    for b in range(blocks):
        fade_ref[2 * b : 2 * b + 2, :] = f_ref[:, b * LANES : (b + 1) * LANES]
    run = fade_ref[...]
    shift = 1
    while shift < CHUNK:
        run = jnp.where(lane % CHUNK >= shift, run * pltpu.roll(run, shift, 1), run)
        shift *= 2
    fade_ref[...] = run
    inv_ref[...] = 1.0 / run

    closed, gain = [], []
    for c in range(2):
        t, h = t_ref[c], h_ref[c]
        eye = lax.broadcasted_iota(jnp.int32, (obs, obs), 0) == lax.broadcasted_iota(
            jnp.int32, (obs, obs), 1
        )
        column = jnp.sum(jnp.where(eye, w_ref[c : c + 1, :], 0.0), axis=1, keepdims=True)
        g = column * h
        q = lax.dot_general(
            t, h, (((1,), (1,)), ((), ())), precision=HIGHEST, preferred_element_type=F32
        )
        closed.append(t - exact_dot(q, g))
        gain.append(g)
        closed_ref[c] = closed[c]
        gain_ref[c] = g
        seen_ref[c] = q

    large.wait()
    row = lax.broadcasted_iota(jnp.int32, (per_block, LANES), 0)
    wide = lax.broadcasted_iota(jnp.int32, (per_block, LANES), 1)
    last = wide == row * CHUNK + (CHUNK - 1)
    for b in range(blocks):
        y = y_ref[:, b * LANES : (b + 1) * LANES]
        top = y[:obs] * inv_ref[2 * b : 2 * b + 1, :]
        bottom = y[obs:] * inv_ref[2 * b + 1 : 2 * b + 2, :]
        turned = jnp.concatenate([top, bottom], axis=0).T
        for r in range(per_block):
            at = (b * per_block + r) * PITCH
            yt_ref[at : at + CHUNK, :] = turned[r * CHUNK : (r + 1) * CHUNK]
        for c in range(2):
            value = jnp.where(last, fade_ref[2 * b + c : 2 * b + c + 1, :], 0.0)
            total = jnp.sum(value, axis=1, keepdims=True)
            phi_ref[c, b * per_block : (b + 1) * per_block, :] = jnp.broadcast_to(
                total, (per_block, LANES)
            )

    low_half = lane < obs
    for p in range(CHUNK // 2):
        even = yt_ref[pl.ds(2 * p, chunks, stride=PITCH), :]
        odd = pltpu.roll(yt_ref[pl.ds(2 * p + 1, chunks, stride=PITCH), :], obs, 1)
        pairs_ref[0, p] = side_by_side(jnp.where(low_half, even, odd))
        pairs_ref[1, p] = side_by_side(jnp.where(low_half, odd, even))

    powers = []
    for c in range(2):
        b1, g = closed[c], gain[c]
        power = squared(b1)
        double_ref[c] = power
        gb = times(g, packed(b1))
        stack = jnp.concatenate([gb, g] if c == 0 else [g, gb], axis=0)
        reach = 2
        while reach < CHUNK:
            stack = jnp.concatenate([times(stack, packed(power)), stack], axis=0)
            power = squared(power)
            reach *= 2
        total = jnp.zeros((chunks, 2 * LANES), F32)
        for p in range(CHUNK // 2):
            both = packed(stack[p * LANES : (p + 1) * LANES])
            total = total + dot(pairs_ref[c, p], jnp.concatenate([both, both], axis=0))
        powers.append(power)
        sums_ref[c] = phi_ref[c] * (total[:, :LANES] + total[:, LANES:])

    levels = chunks.bit_length() - 1
    for level in range(levels):
        half = chunks >> (level + 1)
        for c in range(2):
            both = packed(powers[c])
            powers_ref[c, level] = both
            source, factors = (sums_ref, phi_ref) if level == 0 else (tree_ref, treef_ref)
            base = 0 if level == 0 else chunks - 4 * half
            first = source[c, pl.ds(base, half, stride=2), :]
            second = source[c, pl.ds(base + 1, half, stride=2), :]
            f0 = factors[c, pl.ds(base, half, stride=2), :]
            f1 = factors[c, pl.ds(base + 1, half, stride=2), :]
            state = second + f1 * times(first, both)
            at = chunks - 2 * half
            tree_ref[c, at : at + half, :] = state
            treef_ref[c, at : at + half, :] = f0 * f1
            if level == levels - 1:
                last_ref[c] = powers[c]
                ends_ref[c : c + 1, :] = state
                ends_ref[2 + c : 3 + c, :] = f0 * f1
            else:
                powers[c] = squared(powers[c])


def between(
    sums_ref, phi_ref, pairs_ref, fade_ref, powers_ref, last_ref, closed_ref, double_ref, gain_ref,
    seen_ref,
    scan_ref, cum_ref, square_ref, section_ref, stepx_ref, stepe_ref, partx_ref, parte_ref,
    pad_ref, padf_ref, tmp_ref,
):
    chunks = sums_ref.shape[1]
    blocks = chunks * CHUNK // LANES
    per_block = LANES // CHUNK
    obs = gain_ref.shape[1]

    run = fade_ref[...]
    for r in range(per_block):
        moved = pltpu.roll(run, (LANES - r * CHUNK) % LANES, 1) if r else run
        tmp_ref[...] = moved * moved
        for c in range(2):
            square_ref[c, pl.ds(r, blocks, stride=per_block), :] = tmp_ref[
                pl.ds(c, blocks, stride=2), :
            ]

    weights = []
    for c in range(2):
        section_ref[c] = packed(squared(last_ref[c]))
        b1, b2, g, q = closed_ref[c], double_ref[c], gain_ref[c], seen_ref[c]
        gb, bq, gq = exact_dot(g, b1), exact_dot(b1, q), exact_dot(g, q)
        high, low = halves(jnp.concatenate([b1, b2], axis=1))
        stepx_ref[c] = jnp.concatenate([high, high, low], axis=0)
        both = packed(jnp.concatenate([q, bq], axis=1))
        stepe_ref[c] = jnp.concatenate([both, both], axis=0)
        none = jnp.zeros((obs, obs), F32)
        top = jnp.concatenate([g, gb, none, gq], axis=1)
        bottom = jnp.concatenate([jnp.zeros_like(g), g, none, none], axis=1)
        high, low = halves(jnp.concatenate([top, bottom] if c == 0 else [bottom, top], axis=0))
        weights.append(jnp.concatenate([high, high, low], axis=0))
        pad_ref[c, :LANES, :] = jnp.zeros((LANES, LANES), F32)
        padf_ref[c, :LANES, :] = jnp.ones((LANES, LANES), F32)

    levels = powers_ref.shape[1]
    state = [sums_ref[c] for c in range(2)]
    factor = [phi_ref[c] for c in range(2)]
    for p in range(max(levels, CHUNK // 2)):
        for c in range(2):
            if p < levels:
                reach = 1 << p
                pad_ref[c, LANES:, :] = state[c]
                padf_ref[c, LANES:, :] = factor[c]
                moved = pad_ref[c, pl.ds(LANES - reach, chunks), :]
                state[c] = state[c] + factor[c] * times(moved, powers_ref[c, p])
                factor[c] = factor[c] * padf_ref[c, pl.ds(LANES - reach, chunks), :]
            if p < CHUNK // 2:
                y = pairs_ref[c, p]
                out = dot(jnp.concatenate([y, y[:, :LANES]], axis=1), weights[c])
                observed = y[:, :LANES].astype(F32) + y[:, LANES:].astype(F32)
                if c == 1:
                    observed = pltpu.roll(observed, obs, 1)
                partx_ref[c, p] = out[:, : 2 * LANES]
                parte_ref[c, p] = observed - out[:, 2 * LANES :]
    for c in range(2):
        scan_ref[c] = state[c]
        cum_ref[c] = factor[c]


def after(
    one_ref, two_ref, three_ref, scan_ref, cum_ref, square_ref, section_ref, stepx_ref, stepe_ref,
    partx_ref, parte_ref, powers_ref, weight_ref,
    rows_ref, nis_ref,
    carry_ref, pad_ref, xt_ref, sem,
):
    chunks = scan_ref.shape[1]
    blocks = chunks * CHUNK // LANES
    per_block = LANES // CHUNK
    obs = weight_ref.shape[1]
    levels = powers_ref.shape[1]
    position = lax.axis_index("tm")
    some = [(position >= k).astype(F32) for k in (1, 2, 3)]

    x = []
    for c in range(2):
        section = section_ref[c]
        s = [r[c : c + 1, :] * m for r, m in zip((one_ref, two_ref, three_ref), some)]
        f = [r[2 + c : 3 + c, :] * m for r, m in zip((one_ref, two_ref, three_ref), some)]
        wide = lambda v: jnp.broadcast_to(v, (8, LANES))
        inner = wide(s[1]) + wide(f[1]) * times(wide(s[2]), section)
        entering = wide(s[0]) + wide(f[0]) * times(inner, section)
        carry_ref[c, :8, :] = entering
        for level in range(levels):
            reach = 1 << level
            rows = max(reach, 8)
            moved = times(carry_ref[c, :rows, :], powers_ref[c, level])
            carry_ref[c, pl.ds(reach, rows), :] = moved
        pad_ref[0, :8, :] = jnp.zeros((8, LANES), F32)
        pad_ref[1, :8, :] = jnp.ones((8, LANES), F32)
        pad_ref[0, 8:, :] = scan_ref[c]
        pad_ref[1, 8:, :] = cum_ref[c]
        x.append(
            pad_ref[0, pl.ds(7, chunks), :]
            + pad_ref[1, pl.ds(7, chunks), :] * carry_ref[c, :chunks, :]
        )

    row = lax.broadcasted_iota(jnp.int32, (LANES, LANES), 0)
    col = lax.broadcasted_iota(jnp.int32, (LANES, LANES), 1)
    score = [jnp.zeros((chunks, LANES), F32) for _ in range(2)]
    copies = []
    for p in range(CHUNK // 2):
        for c in range(2):
            both = side_by_side(x[c])
            out = partx_ref[c, p] + dot(
                jnp.concatenate([both, both[:, :LANES]], axis=1), stepx_ref[c]
            )
            seen = dot(both, stepe_ref[c])
            x[c] = out[:, LANES:]
            xt_ref[c, 2 * p] = out[:, :LANES]
            xt_ref[c, 2 * p + 1] = x[c]
            pair = pl.ds(2 * p, 2)
            copy = pltpu.make_async_copy(
                xt_ref.at[c, pair], rows_ref.at[c, pair], sem.at[c, p]
            )
            copy.start()
            copies.append(copy)
            innovation = parte_ref[c, p] - (seen[:, :LANES] + seen[:, LANES:])
            w = weight_ref[c : c + 1, :]
            term = innovation * innovation * jnp.concatenate([w, w], axis=1)
            pick = jnp.where(col == 2 * p + row // obs, 1.0, 0.0).astype(BF16)
            score[c] = score[c] + dot(side_by_side(term), jnp.concatenate([pick, pick], axis=0))

    total = score[0] * square_ref[0] + score[1] * square_ref[1]
    lanes = lax.broadcasted_iota(jnp.int32, (1, LANES), 1)
    total = jnp.where(lanes < CHUNK, total, 0.0)
    per_batch = jnp.sum(total.reshape(blocks, per_block, LANES), axis=1)
    local = lax.dot_general(
        jnp.ones((8, LANES), F32), per_batch, (((1,), (1,)), ((), ())),
        precision=HIGHEST, preferred_element_type=F32,
    )
    nis_ref[...] = jnp.broadcast_to(local[:1][None], nis_ref.shape)
    for copy in copies:
        copy.wait()


def write(rows_ref, fade_ref, out_ref, xt_ref, stage_ref, in_sem, out_sem):
    channels, steps, chunks, _ = rows_ref.shape
    per_block = LANES // CHUNK
    group = 64
    arriving = {}
    for k in range(chunks // group):
        for c in range(channels):
            part = pl.ds(k * group, group)
            arriving[k, c] = pltpu.make_async_copy(
                rows_ref.at[c, :, part], xt_ref.at[c, k], in_sem.at[c, k]
            )
            arriving[k, c].start()
    leaving = []
    for k in range(chunks // group):
        for c in range(channels):
            arriving[k, c].wait()
            flat = xt_ref.at[c, k]
            for b in range(group // per_block):
                tall = jnp.concatenate(
                    [flat[:, b * per_block + i, :] for i in range(per_block)], axis=0
                )
                block = k * (group // per_block) + b
                row = fade_ref[2 * block + c : 2 * block + c + 1, :]
                stage_ref[c, :, block * LANES : (block + 1) * LANES] = tall.T * row
            columns = pl.ds(k * group * CHUNK, group * CHUNK)
            copy = pltpu.make_async_copy(
                stage_ref.at[c, :, columns], out_ref.at[c, :, columns], out_sem.at[c, k]
            )
            copy.start()
            leaving.append(copy)
    for copy in leaving:
        copy.wait()


def per_device(observations, transition, obs_map, measured_weighting, obs_precision, fading):
    channels, obs, frames = observations.shape
    width = transition.shape[1]
    chunks = frames // CHUNK
    levels = chunks.bit_length() - 1
    blocks = frames // LANES
    vmem = pl.BlockSpec(memory_space=pltpu.VMEM)
    spec = jax.ShapeDtypeStruct
    first = [
        spec((2 * channels, width), F32),
        spec((channels, chunks, width), F32),
        spec((channels, chunks, width), F32),
        spec((channels, CHUNK // 2, chunks, 2 * LANES), BF16),
        spec((2 * blocks, LANES), F32),
        spec((channels, levels, width, 2 * width), BF16),
        spec((channels, width, width), F32),
        spec((channels, width, width), F32),
        spec((channels, width, width), F32),
        spec((channels, obs, width), F32),
        spec((channels, width, obs), F32),
    ]
    ends, *kept = pl.pallas_call(
        before,
        out_shape=first,
        in_specs=[pl.BlockSpec(memory_space=pltpu.HBM)] * 5,
        out_specs=[vmem] * len(first),
        scratch_shapes=[
            pltpu.VMEM((chunks * PITCH, LANES), F32),
            pltpu.VMEM((2 * blocks, LANES), F32),
            pltpu.VMEM((channels, chunks, width), F32),
            pltpu.VMEM((channels, chunks, width), F32),
            pltpu.VMEM((channels * obs, frames), F32),
            pltpu.VMEM(fading.shape, F32),
            pltpu.VMEM(transition.shape, F32),
            pltpu.VMEM(obs_map.shape, F32),
            pltpu.VMEM(measured_weighting.shape, F32),
            pltpu.SemaphoreType.DMA((5,)),
        ],
        compiler_params=pltpu.CompilerParams(vmem_limit_bytes=24 << 20),
        name="before",
    )(
        *(
            pltpu.with_memory_space_constraint(a, pltpu.HBM)
            for a in (
                observations.reshape(channels * obs, frames), fading, transition, obs_map,
                measured_weighting,
            )
        )
    )
    fade, powers = kept[3], kept[4]
    second = [
        spec((channels, chunks, width), F32),
        spec((channels, chunks, width), F32),
        spec((channels, chunks, LANES), F32),
        spec((channels, width, 2 * width), BF16),
        spec((channels, 3 * width, 2 * width), BF16),
        spec((channels, 2 * width, 4 * obs), BF16),
        spec((channels, CHUNK // 2, chunks, 2 * width), F32),
        spec((channels, CHUNK // 2, chunks, 2 * obs), F32),
    ]
    made = pl.pallas_call(
        between,
        out_shape=second,
        in_specs=[vmem] * len(kept),
        out_specs=[vmem] * len(second),
        scratch_shapes=[
            pltpu.VMEM((channels, LANES + chunks, width), F32),
            pltpu.VMEM((channels, LANES + chunks, width), F32),
            pltpu.VMEM((2 * blocks, LANES), F32),
        ],
        compiler_params=pltpu.CompilerParams(vmem_limit_bytes=24 << 20),
        cost_estimate=pl.CostEstimate(
            flops=4_000_000_000, bytes_accessed=8_000_000, transcendentals=0
        ),
        name="between",
    )(*kept)
    sections = lax.axis_size("tm")
    arrived = [
        lax.ppermute(ends, "tm", [(i, (i + s) % sections) for i in range(sections)])
        for s in (1, 2, 3)
    ]
    group = lax.axis_size("chan")
    rows, nis = pl.pallas_call(
        after,
        out_shape=[
            pltpu.HBM((channels, CHUNK, chunks, width), F32),
            spec((group, 1, blocks), F32),
        ],
        in_specs=[vmem] * (5 + len(second)),
        out_specs=[pl.BlockSpec(memory_space=pltpu.HBM), vmem],
        scratch_shapes=[
            pltpu.VMEM((channels, chunks + 8, width), F32),
            pltpu.VMEM((2, chunks + 8, width), F32),
            pltpu.VMEM((channels, CHUNK, chunks, width), F32),
            pltpu.SemaphoreType.DMA((channels, CHUNK // 2)),
        ],
        compiler_params=pltpu.CompilerParams(vmem_limit_bytes=24 << 20),
        cost_estimate=pl.CostEstimate(
            flops=4_000_000_000, bytes_accessed=8_000_000, transcendentals=0
        ),
        name="after",
    )(*arrived, *made, powers, obs_precision)
    everything = lax.all_to_all(nis, "chan", split_axis=0, concat_axis=0, tiled=True)
    states = pl.pallas_call(
        write,
        out_shape=jax.ShapeDtypeStruct((channels, width, frames), F32),
        in_specs=[pl.BlockSpec(memory_space=pltpu.HBM), vmem],
        out_specs=pl.BlockSpec(memory_space=pltpu.HBM),
        scratch_shapes=[
            pltpu.VMEM((channels, chunks // 64, CHUNK, 64, width), F32),
            pltpu.VMEM((channels, width, frames), F32),
            pltpu.SemaphoreType.DMA((channels, chunks // 64)),
            pltpu.SemaphoreType.DMA((channels, chunks // 64)),
        ],
        compiler_params=pltpu.CompilerParams(vmem_limit_bytes=16 << 20),
        cost_estimate=pl.CostEstimate(
            flops=4_000_000_000, bytes_accessed=8 * channels * width * frames, transcendentals=0
        ),
        name="write",
    )(pltpu.with_memory_space_constraint(rows, pltpu.HBM), fade)
    divisor = channels * lax.axis_size("chan") * BATCH * obs
    return states, jnp.sum(everything, axis=(0, 1)) / divisor


def solution(mesh):
    in_specs = (
        P("chan", None, "tm"),
        P("chan", None, None),
        P("chan", None, None),
        P("chan", None),
        P("chan", None),
        P("chan", "tm"),
    )
    out_specs = (P("chan", None, "tm"), P("tm"))
    return jax.shard_map(
        per_device, mesh=mesh, in_specs=in_specs, out_specs=out_specs, check_vma=False
    )
```

```python
import jax
import jax.numpy as jnp
from jax import lax
from jax.experimental import pallas as pl
from jax.experimental.pallas import tpu as pltpu
from jax.sharding import PartitionSpec as P

LANES = 128
CHUNK = 16
PITCH = 17
BATCH = 128
F32 = jnp.float32
BF16 = jnp.bfloat16
HIGHEST = lax.Precision.HIGHEST


def dot(a, b):
    return jnp.dot(a, b, preferred_element_type=F32)


def exact_dot(a, b):
    return jnp.dot(a, b, preferred_element_type=F32, precision=HIGHEST)


def halves(x):
    high = x.astype(BF16)
    low = (x - high.astype(F32)).astype(BF16)
    return high, low


def packed(m):
    high, low = halves(m)
    return jnp.concatenate([high, low], axis=1)


def side_by_side(x):
    high, low = halves(x)
    return jnp.concatenate([high, low], axis=1)


def thirds(x):
    first = x.astype(BF16)
    rest = x - first.astype(F32)
    second = rest.astype(BF16)
    return first, second, (rest - second.astype(F32)).astype(BF16)


def squared(x):
    a, b, c = thirds(x)
    pair = jnp.concatenate([a, b], axis=1)
    out = dot(pair, jnp.concatenate([pair, pair], axis=0))
    rest = dot(jnp.concatenate([a, c], axis=1), jnp.concatenate([c, a], axis=0))
    return out[:, :LANES] + (out[:, LANES:] + rest)


def times(x, both):
    weights = jnp.concatenate([both, both], axis=0)
    out = dot(side_by_side(x), weights)
    width = out.shape[1] // 2
    return out[:, :width] + out[:, width:]


def times_rows(x, both):
    rows = x.shape[0]
    high = x.astype(BF16).astype(F32)
    out = dot(jnp.concatenate([high, x - high], axis=0).astype(BF16), both)
    out = out[:rows] + out[rows:]
    return out[:, :LANES] + out[:, LANES:]


def before(
    y_hbm, f_hbm, t_hbm, h_hbm, w_hbm,
    ends_ref, sums_ref, phi_ref, pairs_ref, fade_ref, powers_ref, last_ref, closed_ref, double_ref,
    gain_ref, seen_ref,
    yt_ref, inv_ref, tree_ref, treef_ref, y_ref, f_ref, t_ref, h_ref, w_ref, in_sem,
):
    small = [
        pltpu.make_async_copy(source, target, in_sem.at[k])
        for k, (source, target) in enumerate(
            ((f_hbm, f_ref), (t_hbm, t_ref), (h_hbm, h_ref), (w_hbm, w_ref))
        )
    ]
    large = pltpu.make_async_copy(y_hbm, y_ref, in_sem.at[4])
    for copy in small:
        copy.start()
    large.start()
    for copy in small:
        copy.wait()
    frames = y_ref.shape[1]
    blocks = frames // LANES
    chunks = frames // CHUNK
    per_block = LANES // CHUNK
    obs = h_ref.shape[1]
    lane = lax.broadcasted_iota(jnp.int32, (1, LANES), 1)

    for b in range(blocks):
        fade_ref[2 * b : 2 * b + 2, :] = f_ref[:, b * LANES : (b + 1) * LANES]
    run = fade_ref[...]
    shift = 1
    while shift < CHUNK:
        run = jnp.where(lane % CHUNK >= shift, run * pltpu.roll(run, shift, 1), run)
        shift *= 2
    fade_ref[...] = run
    inv_ref[...] = 1.0 / run

    closed, gain = [], []
    for c in range(2):
        t, h = t_ref[c], h_ref[c]
        eye = lax.broadcasted_iota(jnp.int32, (obs, obs), 0) == lax.broadcasted_iota(
            jnp.int32, (obs, obs), 1
        )
        column = jnp.sum(jnp.where(eye, w_ref[c : c + 1, :], 0.0), axis=1, keepdims=True)
        g = column * h
        q = lax.dot_general(
            t, h, (((1,), (1,)), ((), ())), precision=HIGHEST, preferred_element_type=F32
        )
        closed.append(t - exact_dot(q, g))
        gain.append(g)
        closed_ref[c] = closed[c]
        gain_ref[c] = g
        seen_ref[c] = q

    power = [squared(m) for m in closed]
    stack = []
    for c in range(2):
        double_ref[c] = power[c]
        gb = times(gain[c], packed(closed[c]))
        stack.append(jnp.concatenate([gb, gain[c]] if c == 0 else [gain[c], gb], axis=0))

    levels = chunks.bit_length() - 1
    first_level = CHUNK.bit_length() - 1
    exponent = 1

    def advance():
        nonlocal exponent
        for c in range(2):
            both = packed(power[c])
            if exponent < first_level:
                stack[c] = jnp.concatenate([times(stack[c], both), stack[c]], axis=0)
            else:
                powers_ref[c, exponent - first_level] = both
            if exponent - first_level == levels - 1:
                last_ref[c] = power[c]
            else:
                power[c] = squared(power[c])
        exponent += 1

    large.wait()
    row = lax.broadcasted_iota(jnp.int32, (per_block, LANES), 0)
    wide = lax.broadcasted_iota(jnp.int32, (per_block, LANES), 1)
    last = wide == row * CHUNK + (CHUNK - 1)
    for b in range(blocks):
        y = y_ref[:, b * LANES : (b + 1) * LANES]
        top = y[:obs] * inv_ref[2 * b : 2 * b + 1, :]
        bottom = y[obs:] * inv_ref[2 * b + 1 : 2 * b + 2, :]
        turned = jnp.concatenate([top, bottom], axis=0).T
        for r in range(per_block):
            at = (b * per_block + r) * PITCH
            yt_ref[at : at + CHUNK, :] = turned[r * CHUNK : (r + 1) * CHUNK]
        for c in range(2):
            value = jnp.where(last, fade_ref[2 * b + c : 2 * b + c + 1, :], 0.0)
            total = jnp.sum(value, axis=1, keepdims=True)
            phi_ref[c, b * per_block : (b + 1) * per_block, :] = jnp.broadcast_to(
                total, (per_block, LANES)
            )
        if b % 3 == 1:
            advance()

    low_half = lane < obs
    total = [jnp.zeros((chunks, 2 * LANES), F32) for _ in range(2)]
    for p in range(CHUNK // 2):
        even = yt_ref[pl.ds(2 * p, chunks, stride=PITCH), :]
        odd = pltpu.roll(yt_ref[pl.ds(2 * p + 1, chunks, stride=PITCH), :], obs, 1)
        for c in range(2):
            value = jnp.where(low_half, even, odd) if c == 0 else jnp.where(low_half, odd, even)
            pairs_ref[c, p] = side_by_side(value)
            both = packed(stack[c][p * LANES : (p + 1) * LANES])
            total[c] = total[c] + dot(pairs_ref[c, p], jnp.concatenate([both, both], axis=0))
    for c in range(2):
        sums_ref[c] = phi_ref[c] * (total[c][:, :LANES] + total[c][:, LANES:])

    for level in range(levels):
        half = chunks >> (level + 1)
        rows = max(half, 8)
        source, factors = (sums_ref, phi_ref) if level == 0 else (tree_ref, treef_ref)
        base = 0 if level == 0 else chunks - 4 * half
        at = chunks - 2 * half
        for c in range(2):
            first = source[c, pl.ds(base, rows, stride=2), :]
            second = source[c, pl.ds(base + 1, rows, stride=2), :]
            f0 = factors[c, pl.ds(base, rows, stride=2), :]
            f1 = factors[c, pl.ds(base + 1, rows, stride=2), :]
            state = second + f1 * times_rows(first, powers_ref[c, level])
            factor = f0 * f1
            if level == levels - 1:
                ends_ref[c : c + 1, :] = state[:1]
                ends_ref[2 + c : 3 + c, :] = factor[:1]
            else:
                tree_ref[c, at : at + half, :] = state[:half]
                treef_ref[c, at : at + half, :] = factor[:half]


def between(
    sums_ref, phi_ref, pairs_ref, fade_ref, powers_ref, last_ref, closed_ref, double_ref, gain_ref,
    seen_ref,
    scan_ref, cum_ref, square_ref, section_ref, stepx_ref, stepe_ref, partx_ref, parte_ref,
    pad_ref, padf_ref, tmp_ref,
):
    chunks = sums_ref.shape[1]
    blocks = chunks * CHUNK // LANES
    per_block = LANES // CHUNK
    obs = gain_ref.shape[1]

    run = fade_ref[...]
    for r in range(per_block):
        moved = pltpu.roll(run, (LANES - r * CHUNK) % LANES, 1) if r else run
        tmp_ref[...] = moved * moved
        for c in range(2):
            square_ref[c, pl.ds(r, blocks, stride=per_block), :] = tmp_ref[
                pl.ds(c, blocks, stride=2), :
            ]

    weights = []
    for c in range(2):
        section_ref[c] = packed(squared(last_ref[c]))
        b1, b2, g, q = closed_ref[c], double_ref[c], gain_ref[c], seen_ref[c]
        gb, bq, gq = exact_dot(g, b1), exact_dot(b1, q), exact_dot(g, q)
        high, low = halves(jnp.concatenate([b1, b2], axis=1))
        stepx_ref[c] = jnp.concatenate([high, high, low], axis=0)
        both = packed(jnp.concatenate([q, bq], axis=1))
        stepe_ref[c] = jnp.concatenate([both, both], axis=0)
        none = jnp.zeros((obs, obs), F32)
        top = jnp.concatenate([g, gb, none, gq], axis=1)
        bottom = jnp.concatenate([jnp.zeros_like(g), g, none, none], axis=1)
        high, low = halves(jnp.concatenate([top, bottom] if c == 0 else [bottom, top], axis=0))
        weights.append(jnp.concatenate([high, high, low], axis=0))
        pad_ref[c, :LANES, :] = jnp.zeros((LANES, LANES), F32)
        padf_ref[c, :LANES, :] = jnp.ones((LANES, LANES), F32)

    levels = powers_ref.shape[1]
    state = [sums_ref[c] for c in range(2)]
    factor = [phi_ref[c] for c in range(2)]
    for p in range(max(levels, CHUNK // 2)):
        for c in range(2):
            if p < levels:
                reach = 1 << p
                pad_ref[c, LANES:, :] = state[c]
                padf_ref[c, LANES:, :] = factor[c]
                moved = pad_ref[c, pl.ds(LANES - reach, chunks), :]
                state[c] = state[c] + factor[c] * times(moved, powers_ref[c, p])
                factor[c] = factor[c] * padf_ref[c, pl.ds(LANES - reach, chunks), :]
            if p < CHUNK // 2:
                y = pairs_ref[c, p]
                out = dot(jnp.concatenate([y, y[:, :LANES]], axis=1), weights[c])
                observed = y[:, :LANES].astype(F32) + y[:, LANES:].astype(F32)
                if c == 1:
                    observed = pltpu.roll(observed, obs, 1)
                partx_ref[c, p] = out[:, : 2 * LANES]
                parte_ref[c, p] = observed - out[:, 2 * LANES :]
    for c in range(2):
        scan_ref[c] = state[c]
        cum_ref[c] = factor[c]


def after(
    one_ref, two_ref, three_ref, scan_ref, cum_ref, square_ref, section_ref, stepx_ref, stepe_ref,
    partx_ref, parte_ref, powers_ref, weight_ref,
    rows_ref, nis_ref,
    carry_ref, pad_ref, xt_ref, sem,
):
    chunks = scan_ref.shape[1]
    blocks = chunks * CHUNK // LANES
    per_block = LANES // CHUNK
    obs = weight_ref.shape[1]
    levels = powers_ref.shape[1]
    position = lax.axis_index("tm")
    some = [(position >= k).astype(F32) for k in (1, 2, 3)]

    wide = lambda v: jnp.broadcast_to(v, (8, LANES))
    arrived = (one_ref, two_ref, three_ref)
    s = [[wide(r[c : c + 1, :] * m) for r, m in zip(arrived, some)] for c in range(2)]
    f = [[wide(r[2 + c : 3 + c, :] * m) for r, m in zip(arrived, some)] for c in range(2)]
    entering = [s[c][2] for c in range(2)]
    for k in (1, 0):
        for c in range(2):
            entering[c] = s[c][k] + f[c][k] * times_rows(entering[c], section_ref[c])
    for c in range(2):
        carry_ref[c, :8, :] = entering[c]
        pad_ref[c, 0, :8, :] = jnp.zeros((8, LANES), F32)
        pad_ref[c, 1, :8, :] = jnp.ones((8, LANES), F32)
        pad_ref[c, 0, 8:, :] = scan_ref[c]
        pad_ref[c, 1, 8:, :] = cum_ref[c]
    for level in range(levels):
        reach = 1 << level
        rows = max(reach, 8)
        for c in range(2):
            carry_ref[c, pl.ds(reach, rows), :] = times_rows(
                carry_ref[c, :rows, :], powers_ref[c, level]
            )
    x = [
        pad_ref[c, 0, pl.ds(7, chunks), :]
        + pad_ref[c, 1, pl.ds(7, chunks), :] * carry_ref[c, :chunks, :]
        for c in range(2)
    ]

    row = lax.broadcasted_iota(jnp.int32, (LANES, LANES), 0)
    col = lax.broadcasted_iota(jnp.int32, (LANES, LANES), 1)
    score = [jnp.zeros((chunks, LANES), F32) for _ in range(2)]
    copies = []
    waiting = [None, None]

    def settle(c):
        p, seen = waiting[c]
        innovation = parte_ref[c, p] - (seen[:, :LANES] + seen[:, LANES:])
        w = weight_ref[c : c + 1, :]
        term = innovation * innovation * jnp.concatenate([w, w], axis=1)
        pick = jnp.where(col == 2 * p + row // obs, 1.0, 0.0).astype(BF16)
        score[c] = score[c] + dot(side_by_side(term), jnp.concatenate([pick, pick], axis=0))

    for p in range(CHUNK // 2):
        both = [side_by_side(x[c]) for c in range(2)]
        out = [
            dot(jnp.concatenate([both[c], both[c][:, :LANES]], axis=1), stepx_ref[c])
            for c in range(2)
        ]
        if p:
            for c in range(2):
                settle(c)
        for c in range(2):
            waiting[c] = p, dot(both[c], stepe_ref[c])
        for c in range(2):
            x[c] = partx_ref[c, p, :, LANES:] + out[c][:, LANES:]
            xt_ref[c, 2 * p] = partx_ref[c, p, :, :LANES] + out[c][:, :LANES]
            xt_ref[c, 2 * p + 1] = x[c]
            pair = pl.ds(2 * p, 2)
            copy = pltpu.make_async_copy(
                xt_ref.at[c, pair], rows_ref.at[c, pair], sem.at[c, p]
            )
            copy.start()
            copies.append(copy)
    for c in range(2):
        settle(c)

    total = score[0] * square_ref[0] + score[1] * square_ref[1]
    lanes = lax.broadcasted_iota(jnp.int32, (1, LANES), 1)
    total = jnp.where(lanes < CHUNK, total, 0.0)
    per_batch = jnp.sum(total.reshape(blocks, per_block, LANES), axis=1)
    local = lax.dot_general(
        jnp.ones((8, LANES), F32), per_batch, (((1,), (1,)), ((), ())),
        precision=HIGHEST, preferred_element_type=F32,
    )
    divisor = 2 * nis_ref.shape[0] * BATCH * obs
    nis_ref[...] = jnp.broadcast_to((local[:1] / divisor)[None], nis_ref.shape)
    for copy in copies:
        copy.wait()


def write(rows_ref, fade_ref, out_ref, xt_ref, stage_ref, in_sem, out_sem):
    channels, steps, chunks, _ = rows_ref.shape
    per_block = LANES // CHUNK
    group = 64
    arriving = {}
    for k in range(chunks // group):
        for c in range(channels):
            part = pl.ds(k * group, group)
            arriving[k, c] = pltpu.make_async_copy(
                rows_ref.at[c, :, part], xt_ref.at[c, k], in_sem.at[c, k]
            )
            arriving[k, c].start()
    leaving = []
    for k in range(chunks // group):
        for c in range(channels):
            arriving[k, c].wait()
            flat = xt_ref.at[c, k]
            for b in range(group // per_block):
                tall = jnp.concatenate(
                    [flat[:, b * per_block + i, :] for i in range(per_block)], axis=0
                )
                block = k * (group // per_block) + b
                row = fade_ref[2 * block + c : 2 * block + c + 1, :]
                stage_ref[c, :, block * LANES : (block + 1) * LANES] = tall.T * row
            columns = pl.ds(k * group * CHUNK, group * CHUNK)
            copy = pltpu.make_async_copy(
                stage_ref.at[c, :, columns], out_ref.at[c, :, columns], out_sem.at[c, k]
            )
            copy.start()
            leaving.append(copy)
    for copy in leaving:
        copy.wait()


def per_device(observations, transition, obs_map, measured_weighting, obs_precision, fading):
    channels, obs, frames = observations.shape
    width = transition.shape[1]
    chunks = frames // CHUNK
    levels = chunks.bit_length() - 1
    blocks = frames // LANES
    vmem = pl.BlockSpec(memory_space=pltpu.VMEM)
    spec = jax.ShapeDtypeStruct
    first = [
        spec((2 * channels, width), F32),
        spec((channels, chunks, width), F32),
        spec((channels, chunks, width), F32),
        spec((channels, CHUNK // 2, chunks, 2 * LANES), BF16),
        spec((2 * blocks, LANES), F32),
        spec((channels, levels, width, 2 * width), BF16),
        spec((channels, width, width), F32),
        spec((channels, width, width), F32),
        spec((channels, width, width), F32),
        spec((channels, obs, width), F32),
        spec((channels, width, obs), F32),
    ]
    ends, *kept = pl.pallas_call(
        before,
        out_shape=first,
        in_specs=[pl.BlockSpec(memory_space=pltpu.HBM)] * 5,
        out_specs=[vmem] * len(first),
        scratch_shapes=[
            pltpu.VMEM((chunks * PITCH, LANES), F32),
            pltpu.VMEM((2 * blocks, LANES), F32),
            pltpu.VMEM((channels, chunks + 16, width), F32),
            pltpu.VMEM((channels, chunks + 16, width), F32),
            pltpu.VMEM((channels * obs, frames), F32),
            pltpu.VMEM(fading.shape, F32),
            pltpu.VMEM(transition.shape, F32),
            pltpu.VMEM(obs_map.shape, F32),
            pltpu.VMEM(measured_weighting.shape, F32),
            pltpu.SemaphoreType.DMA((5,)),
        ],
        compiler_params=pltpu.CompilerParams(vmem_limit_bytes=24 << 20),
        name="before",
    )(
        *(
            pltpu.with_memory_space_constraint(a, pltpu.HBM)
            for a in (
                observations.reshape(channels * obs, frames), fading, transition, obs_map,
                measured_weighting,
            )
        )
    )
    fade, powers = kept[3], kept[4]
    second = [
        spec((channels, chunks, width), F32),
        spec((channels, chunks, width), F32),
        spec((channels, chunks, LANES), F32),
        spec((channels, width, 2 * width), BF16),
        spec((channels, 3 * width, 2 * width), BF16),
        spec((channels, 2 * width, 4 * obs), BF16),
        spec((channels, CHUNK // 2, chunks, 2 * width), F32),
        spec((channels, CHUNK // 2, chunks, 2 * obs), F32),
    ]
    made = pl.pallas_call(
        between,
        out_shape=second,
        in_specs=[vmem] * len(kept),
        out_specs=[vmem] * len(second),
        scratch_shapes=[
            pltpu.VMEM((channels, LANES + chunks, width), F32),
            pltpu.VMEM((channels, LANES + chunks, width), F32),
            pltpu.VMEM((2 * blocks, LANES), F32),
        ],
        compiler_params=pltpu.CompilerParams(vmem_limit_bytes=24 << 20),
        cost_estimate=pl.CostEstimate(
            flops=4_000_000_000, bytes_accessed=8_000_000, transcendentals=0
        ),
        name="between",
    )(*kept)
    sections = lax.axis_size("tm")
    arrived = [
        lax.ppermute(ends, "tm", [(i, (i + s) % sections) for i in range(sections)])
        for s in (1, 2, 3)
    ]
    group = lax.axis_size("chan")
    rows, nis = pl.pallas_call(
        after,
        out_shape=[
            pltpu.HBM((channels, CHUNK, chunks, width), F32),
            spec((group, 1, blocks), F32),
        ],
        in_specs=[vmem] * (5 + len(second)),
        out_specs=[pl.BlockSpec(memory_space=pltpu.HBM), vmem],
        scratch_shapes=[
            pltpu.VMEM((channels, chunks + 8, width), F32),
            pltpu.VMEM((channels, 2, chunks + 8, width), F32),
            pltpu.VMEM((channels, CHUNK, chunks, width), F32),
            pltpu.SemaphoreType.DMA((channels, CHUNK // 2)),
        ],
        compiler_params=pltpu.CompilerParams(vmem_limit_bytes=24 << 20),
        cost_estimate=pl.CostEstimate(
            flops=4_000_000_000, bytes_accessed=8_000_000, transcendentals=0
        ),
        name="after",
    )(*arrived, *made, powers, obs_precision)
    everything = lax.all_to_all(nis, "chan", split_axis=0, concat_axis=0, tiled=True)
    states = pl.pallas_call(
        write,
        out_shape=jax.ShapeDtypeStruct((channels, width, frames), F32),
        in_specs=[pl.BlockSpec(memory_space=pltpu.HBM), vmem],
        out_specs=pl.BlockSpec(memory_space=pltpu.HBM),
        scratch_shapes=[
            pltpu.VMEM((channels, chunks // 64, CHUNK, 64, width), F32),
            pltpu.VMEM((channels, width, frames), F32),
            pltpu.SemaphoreType.DMA((channels, chunks // 64)),
            pltpu.SemaphoreType.DMA((channels, chunks // 64)),
        ],
        compiler_params=pltpu.CompilerParams(vmem_limit_bytes=16 << 20),
        cost_estimate=pl.CostEstimate(
            flops=4_000_000_000, bytes_accessed=8 * channels * width * frames, transcendentals=0
        ),
        name="write",
    )(pltpu.with_memory_space_constraint(rows, pltpu.HBM), fade)
    return states, jnp.sum(everything, axis=(0, 1))


def solution(mesh):
    in_specs = (
        P("chan", None, "tm"),
        P("chan", None, None),
        P("chan", None, None),
        P("chan", None),
        P("chan", None),
        P("chan", "tm"),
    )
    out_specs = (P("chan", None, "tm"), P("tm"))
    return jax.shard_map(
        per_device, mesh=mesh, in_specs=in_specs, out_specs=out_specs, check_vma=False
    )
```

```python
import jax
import jax.numpy as jnp
from jax import lax
from jax.experimental import pallas as pl
from jax.experimental.pallas import tpu as pltpu
from jax.sharding import PartitionSpec as P

LANES = 128
CHUNK = 16
PITCH = 17
BATCH = 128
F32 = jnp.float32
BF16 = jnp.bfloat16
HIGHEST = lax.Precision.HIGHEST


def dot(a, b):
    return jnp.dot(a, b, preferred_element_type=F32)


def exact_dot(a, b):
    return jnp.dot(a, b, preferred_element_type=F32, precision=HIGHEST)


def halves(x):
    high = x.astype(BF16)
    low = (x - high.astype(F32)).astype(BF16)
    return high, low


def packed(m):
    high, low = halves(m)
    return jnp.concatenate([high, low], axis=1)


def side_by_side(x):
    high, low = halves(x)
    return jnp.concatenate([high, low], axis=1)


def thirds(x):
    first = x.astype(BF16)
    rest = x - first.astype(F32)
    second = rest.astype(BF16)
    return first, second, (rest - second.astype(F32)).astype(BF16)


def squared(x):
    a, b, c = thirds(x)
    pair = jnp.concatenate([a, b], axis=1)
    out = dot(pair, jnp.concatenate([pair, pair], axis=0))
    rest = dot(jnp.concatenate([a, c], axis=1), jnp.concatenate([c, a], axis=0))
    return out[:, :LANES] + (out[:, LANES:] + rest)


def times(x, both):
    weights = jnp.concatenate([both, both], axis=0)
    out = dot(side_by_side(x), weights)
    width = out.shape[1] // 2
    return out[:, :width] + out[:, width:]


def times_rows(x, both):
    return folded(dot(stacked(x), both))


def stacked(x):
    high = x.astype(BF16).astype(F32)
    return jnp.concatenate([high, x - high], axis=0).astype(BF16)


def folded(out):
    rows = out.shape[0] // 2
    out = out[:rows] + out[rows:]
    return out[:, :LANES] + out[:, LANES:]


def before(
    y_hbm, f_hbm, t_hbm, h_hbm, w_hbm,
    ends_ref, sums_ref, phi_ref, pairs_ref, fade_ref, powers_ref, last_ref, closed_ref, double_ref,
    gain_ref, seen_ref, triple_ref,
    yt_ref, inv_ref, tree_ref, treef_ref, y_ref, f_ref, t_ref, h_ref, w_ref, in_sem,
):
    small = [
        pltpu.make_async_copy(source, target, in_sem.at[k])
        for k, (source, target) in enumerate(
            ((f_hbm, f_ref), (t_hbm, t_ref), (h_hbm, h_ref), (w_hbm, w_ref))
        )
    ]
    large = pltpu.make_async_copy(y_hbm, y_ref, in_sem.at[4])
    for copy in small:
        copy.start()
    large.start()
    for copy in small:
        copy.wait()
    frames = y_ref.shape[1]
    blocks = frames // LANES
    chunks = frames // CHUNK
    per_block = LANES // CHUNK
    obs = h_ref.shape[1]
    lane = lax.broadcasted_iota(jnp.int32, (1, LANES), 1)

    for b in range(blocks):
        fade_ref[2 * b : 2 * b + 2, :] = f_ref[:, b * LANES : (b + 1) * LANES]
    run = fade_ref[...]
    shift = 1
    while shift < CHUNK:
        run = jnp.where(lane % CHUNK >= shift, run * pltpu.roll(run, shift, 1), run)
        shift *= 2
    fade_ref[...] = run
    inv_ref[...] = 1.0 / run

    half_lane = lane < obs
    closed, gain, seen = [None, None], [None, None], [None, None]

    def first_step():
        for c in range(2):
            t, h = t_ref[c], h_ref[c]
            eye = lax.broadcasted_iota(jnp.int32, (obs, obs), 0) == lax.broadcasted_iota(
                jnp.int32, (obs, obs), 1
            )
            column = jnp.sum(jnp.where(eye, w_ref[c : c + 1, :], 0.0), axis=1, keepdims=True)
            gain[c] = column * h
            gain_ref[c] = gain[c]
            t1, t2, t3 = thirds(t)
            h1, h2, h3 = thirds(jnp.concatenate([h, h], axis=0))
            seen[c] = lax.dot_general(
                jnp.concatenate([t1, t1, t1, t2, t2, t3], axis=1),
                jnp.concatenate([h1, h2, h3, h1, h2, h1], axis=1),
                (((1,), (1,)), ((), ())),
                preferred_element_type=F32,
            )
            seen_ref[c] = seen[c][:, :obs]

    def second_step():
        for c in range(2):
            q1, q2, q3 = (v.astype(F32) for v in thirds(seen[c]))
            mixed = jnp.where(half_lane, q1, q3)
            g1, g2, g3 = thirds(gain[c])
            closed[c] = t_ref[c] - dot(
                jnp.concatenate([q1, q2, mixed], axis=1).astype(BF16),
                jnp.concatenate([g1, g2, g1, g2, g3, g1], axis=0),
            )
            closed_ref[c] = closed[c]

    power, stack = [None, None], [None, None]

    def third_step():
        for c in range(2):
            power[c] = squared(closed[c])
            double_ref[c] = power[c]
            gb = times(gain[c], packed(closed[c]))
            stack[c] = jnp.concatenate([gb, gain[c]] if c == 0 else [gain[c], gb], axis=0)

    levels = chunks.bit_length() - 1
    first_level = CHUNK.bit_length() - 1
    exponent = 1
    below = [None, None]

    def advance():
        nonlocal exponent
        for c in range(2):
            both = packed(power[c])
            if exponent < first_level:
                stack[c] = jnp.concatenate([times(stack[c], both), stack[c]], axis=0)
            else:
                level = exponent - first_level
                powers_ref[c, level] = both
                if level % 2:
                    triple_ref[c, level // 2] = packed(times(below[c], both))
                below[c] = power[c]
            if exponent - first_level == levels - 1:
                last_ref[c] = power[c]
            else:
                power[c] = squared(power[c])
        exponent += 1

    first_step()
    second_step()
    third_step()
    large.wait()
    steps = [advance] * (levels + first_level - 1)
    row = lax.broadcasted_iota(jnp.int32, (per_block, LANES), 0)
    wide = lax.broadcasted_iota(jnp.int32, (per_block, LANES), 1)
    last = wide == row * CHUNK + (CHUNK - 1)
    for b in range(blocks):
        y = y_ref[:, b * LANES : (b + 1) * LANES]
        top = y[:obs] * inv_ref[2 * b : 2 * b + 1, :]
        bottom = y[obs:] * inv_ref[2 * b + 1 : 2 * b + 2, :]
        turned = jnp.concatenate([top, bottom], axis=0).T
        for r in range(per_block):
            at = (b * per_block + r) * PITCH
            yt_ref[at : at + CHUNK, :] = turned[r * CHUNK : (r + 1) * CHUNK]
        for c in range(2):
            value = jnp.where(last, fade_ref[2 * b + c : 2 * b + c + 1, :], 0.0)
            total = jnp.sum(value, axis=1, keepdims=True)
            phi_ref[c, b * per_block : (b + 1) * per_block, :] = jnp.broadcast_to(
                total, (per_block, LANES)
            )
        if b % 3 == 1 and steps:
            steps.pop(0)()

    for step in steps:
        step()

    low_half = lane < obs
    total = [jnp.zeros((chunks, 2 * LANES), F32) for _ in range(2)]
    for p in range(CHUNK // 2):
        even = yt_ref[pl.ds(2 * p, chunks, stride=PITCH), :]
        odd = pltpu.roll(yt_ref[pl.ds(2 * p + 1, chunks, stride=PITCH), :], obs, 1)
        for c in range(2):
            value = jnp.where(low_half, even, odd) if c == 0 else jnp.where(low_half, odd, even)
            pairs_ref[c, p] = side_by_side(value)
            both = packed(stack[c][p * LANES : (p + 1) * LANES])
            total[c] = total[c] + dot(pairs_ref[c, p], jnp.concatenate([both, both], axis=0))
    for c in range(2):
        sums_ref[c] = phi_ref[c] * (total[c][:, :LANES] + total[c][:, LANES:])

    source, factors, base, at = sums_ref, phi_ref, 0, 0
    for level in range(levels // 2):
        count = chunks >> (2 * level + 2)
        rows = max(count, 8)
        for c in range(2):
            e = [source[c, pl.ds(base + k, rows, stride=4), :] for k in range(4)]
            f = [factors[c, pl.ds(base + k, rows, stride=4), :] for k in range(4)]
            f2 = f[3] * f[2]
            f1 = f2 * f[1]
            weights = jnp.concatenate(
                [powers_ref[c, 2 * level], powers_ref[c, 2 * level + 1], triple_ref[c, level]],
                axis=0,
            )
            moved = jnp.concatenate([e[2] * f[3], e[1] * f2, e[0] * f1], axis=1)
            state = e[3] + folded(dot(stacked(moved), weights))
            factor = f1 * f[0]
            if level == levels // 2 - 1:
                ends_ref[c : c + 1, :] = state[:1]
                ends_ref[2 + c : 3 + c, :] = factor[:1]
            else:
                tree_ref[c, at : at + count, :] = state[:count]
                treef_ref[c, at : at + count, :] = factor[:count]
        source, factors, base = tree_ref, treef_ref, at
        at += count


def between(
    sums_ref, phi_ref, pairs_ref, fade_ref, powers_ref, last_ref, closed_ref, double_ref, gain_ref,
    seen_ref,
    scan_ref, cum_ref, square_ref, section_ref, stepx_ref, stepe_ref, partx_ref, parte_ref,
    pad_ref, padf_ref, tmp_ref,
):
    chunks = sums_ref.shape[1]
    blocks = chunks * CHUNK // LANES
    per_block = LANES // CHUNK
    obs = gain_ref.shape[1]

    run = fade_ref[...]
    for r in range(per_block):
        moved = pltpu.roll(run, (LANES - r * CHUNK) % LANES, 1) if r else run
        tmp_ref[...] = moved * moved
        for c in range(2):
            square_ref[c, pl.ds(r, blocks, stride=per_block), :] = tmp_ref[
                pl.ds(c, blocks, stride=2), :
            ]

    weights = []
    for c in range(2):
        section = squared(last_ref[c])
        section_ref[c] = jnp.concatenate([packed(section), packed(squared(section))], axis=0)
        b1, b2, g, q = closed_ref[c], double_ref[c], gain_ref[c], seen_ref[c]
        gb, bq, gq = exact_dot(g, b1), exact_dot(b1, q), exact_dot(g, q)
        high, low = halves(jnp.concatenate([b1, b2], axis=1))
        stepx_ref[c] = jnp.concatenate([high, high, low], axis=0)
        both = packed(jnp.concatenate([q, bq], axis=1))
        stepe_ref[c] = jnp.concatenate([both, both], axis=0)
        none = jnp.zeros((obs, obs), F32)
        top = jnp.concatenate([g, gb, none, gq], axis=1)
        bottom = jnp.concatenate([jnp.zeros_like(g), g, none, none], axis=1)
        high, low = halves(jnp.concatenate([top, bottom] if c == 0 else [bottom, top], axis=0))
        weights.append(jnp.concatenate([high, high, low], axis=0))
        pad_ref[c, :LANES, :] = jnp.zeros((LANES, LANES), F32)
        padf_ref[c, :LANES, :] = jnp.ones((LANES, LANES), F32)

    levels = powers_ref.shape[1]
    state = [sums_ref[c] for c in range(2)]
    factor = [phi_ref[c] for c in range(2)]
    for p in range(max(levels, CHUNK // 2)):
        for c in range(2):
            if p < levels:
                reach = 1 << p
                pad_ref[c, LANES:, :] = state[c]
                padf_ref[c, LANES:, :] = factor[c]
                moved = pad_ref[c, pl.ds(LANES - reach, chunks), :]
                state[c] = state[c] + factor[c] * times(moved, powers_ref[c, p])
                factor[c] = factor[c] * padf_ref[c, pl.ds(LANES - reach, chunks), :]
            if p < CHUNK // 2:
                y = pairs_ref[c, p]
                out = dot(jnp.concatenate([y, y[:, :LANES]], axis=1), weights[c])
                observed = y[:, :LANES].astype(F32) + y[:, LANES:].astype(F32)
                if c == 1:
                    observed = pltpu.roll(observed, obs, 1)
                partx_ref[c, p] = out[:, : 2 * LANES]
                parte_ref[c, p] = observed - out[:, 2 * LANES :]
    for c in range(2):
        scan_ref[c] = state[c]
        cum_ref[c] = factor[c]


def after(
    one_ref, two_ref, three_ref, scan_ref, cum_ref, square_ref, section_ref, stepx_ref, stepe_ref,
    partx_ref, parte_ref, powers_ref, triple_ref, weight_ref,
    rows_ref, nis_ref,
    carry_ref, pad_ref, xt_ref, sem,
):
    chunks = scan_ref.shape[1]
    blocks = chunks * CHUNK // LANES
    per_block = LANES // CHUNK
    obs = weight_ref.shape[1]
    levels = powers_ref.shape[1]
    position = lax.axis_index("tm")
    some = [(position >= k).astype(F32) for k in (1, 2, 3)]

    wide = lambda v: jnp.broadcast_to(v, (8, LANES))
    arrived = (one_ref, two_ref, three_ref)
    s = [[wide(r[c : c + 1, :] * m) for r, m in zip(arrived, some)] for c in range(2)]
    f = [[wide(r[2 + c : 3 + c, :] * m) for r, m in zip(arrived, some)] for c in range(2)]
    entering = []
    for c in range(2):
        earlier = jnp.concatenate([f[c][0] * s[c][1], f[c][0] * f[c][1] * s[c][2]], axis=1)
        entering.append(s[c][0] + folded(dot(stacked(earlier), section_ref[c])))
    for c in range(2):
        carry_ref[c, :8, :] = entering[c]
        pad_ref[c, 0, :8, :] = jnp.zeros((8, LANES), F32)
        pad_ref[c, 1, :8, :] = jnp.ones((8, LANES), F32)
        pad_ref[c, 0, 8:, :] = scan_ref[c]
        pad_ref[c, 1, 8:, :] = cum_ref[c]
    for level in range(levels // 2):
        reach = 1 << (2 * level)
        rows = max(reach, 8)
        for c in range(2):
            few = stacked(carry_ref[c, :rows, :])
            weights = (powers_ref[c, 2 * level], powers_ref[c, 2 * level + 1], triple_ref[c, level])
            moved = [folded(dot(few, m)) for m in weights]
            for k in range(3):
                carry_ref[c, pl.ds((k + 1) * reach, rows), :] = moved[k]
    x = [
        pad_ref[c, 0, pl.ds(7, chunks), :]
        + pad_ref[c, 1, pl.ds(7, chunks), :] * carry_ref[c, :chunks, :]
        for c in range(2)
    ]

    row = lax.broadcasted_iota(jnp.int32, (LANES, LANES), 0)
    col = lax.broadcasted_iota(jnp.int32, (LANES, LANES), 1)
    score = [jnp.zeros((chunks, LANES), F32) for _ in range(2)]
    copies = []
    waiting = [None, None]

    def settle(c):
        p, seen = waiting[c]
        innovation = parte_ref[c, p] - (seen[:, :LANES] + seen[:, LANES:])
        w = weight_ref[c : c + 1, :]
        term = innovation * innovation * jnp.concatenate([w, w], axis=1)
        pick = jnp.where(col == 2 * p + row // obs, 1.0, 0.0).astype(BF16)
        score[c] = score[c] + dot(side_by_side(term), jnp.concatenate([pick, pick], axis=0))

    for p in range(CHUNK // 2):
        both = [side_by_side(x[c]) for c in range(2)]
        out = [
            dot(jnp.concatenate([both[c], both[c][:, :LANES]], axis=1), stepx_ref[c])
            for c in range(2)
        ]
        if p:
            for c in range(2):
                settle(c)
        for c in range(2):
            waiting[c] = p, dot(both[c], stepe_ref[c])
        for c in range(2):
            x[c] = partx_ref[c, p, :, LANES:] + out[c][:, LANES:]
            xt_ref[c, 2 * p] = partx_ref[c, p, :, :LANES] + out[c][:, :LANES]
            xt_ref[c, 2 * p + 1] = x[c]
            pair = pl.ds(2 * p, 2)
            copy = pltpu.make_async_copy(
                xt_ref.at[c, pair], rows_ref.at[c, pair], sem.at[c, p]
            )
            copy.start()
            copies.append(copy)
    for c in range(2):
        settle(c)

    total = score[0] * square_ref[0] + score[1] * square_ref[1]
    lanes = lax.broadcasted_iota(jnp.int32, (1, LANES), 1)
    total = jnp.where(lanes < CHUNK, total, 0.0)
    per_batch = jnp.sum(total.reshape(blocks, per_block, LANES), axis=1)
    local = lax.dot_general(
        jnp.ones((8, 3 * LANES), BF16), jnp.concatenate(thirds(per_batch), axis=1),
        (((1,), (1,)), ((), ())), preferred_element_type=F32,
    )
    divisor = 2 * nis_ref.shape[0] * BATCH * obs
    nis_ref[...] = jnp.broadcast_to((local[:1] / divisor)[None], nis_ref.shape)
    for copy in copies:
        copy.wait()


def write(rows_ref, fade_ref, out_ref, xt_ref, stage_ref, in_sem, out_sem):
    channels, steps, chunks, _ = rows_ref.shape
    per_block = LANES // CHUNK
    group = 64
    arriving = {}
    for k in range(chunks // group):
        for c in range(channels):
            part = pl.ds(k * group, group)
            arriving[k, c] = pltpu.make_async_copy(
                rows_ref.at[c, :, part], xt_ref.at[c, k], in_sem.at[c, k]
            )
            arriving[k, c].start()
    leaving = []
    for k in range(chunks // group):
        for c in range(channels):
            arriving[k, c].wait()
            flat = xt_ref.at[c, k]
            for b in range(group // per_block):
                tall = jnp.concatenate(
                    [flat[:, b * per_block + i, :] for i in range(per_block)], axis=0
                )
                block = k * (group // per_block) + b
                row = fade_ref[2 * block + c : 2 * block + c + 1, :]
                stage_ref[c, :, block * LANES : (block + 1) * LANES] = tall.T * row
            columns = pl.ds(k * group * CHUNK, group * CHUNK)
            copy = pltpu.make_async_copy(
                stage_ref.at[c, :, columns], out_ref.at[c, :, columns], out_sem.at[c, k]
            )
            copy.start()
            leaving.append(copy)
    for copy in leaving:
        copy.wait()


def per_device(observations, transition, obs_map, measured_weighting, obs_precision, fading):
    channels, obs, frames = observations.shape
    width = transition.shape[1]
    chunks = frames // CHUNK
    levels = chunks.bit_length() - 1
    blocks = frames // LANES
    vmem = pl.BlockSpec(memory_space=pltpu.VMEM)
    spec = jax.ShapeDtypeStruct
    first = [
        spec((2 * channels, width), F32),
        spec((channels, chunks, width), F32),
        spec((channels, chunks, width), F32),
        spec((channels, CHUNK // 2, chunks, 2 * LANES), BF16),
        spec((2 * blocks, LANES), F32),
        spec((channels, levels, width, 2 * width), BF16),
        spec((channels, width, width), F32),
        spec((channels, width, width), F32),
        spec((channels, width, width), F32),
        spec((channels, obs, width), F32),
        spec((channels, width, obs), F32),
        spec((channels, levels // 2, width, 2 * width), BF16),
    ]
    ends, *kept, triples = pl.pallas_call(
        before,
        out_shape=first,
        in_specs=[pl.BlockSpec(memory_space=pltpu.HBM)] * 5,
        out_specs=[vmem] * len(first),
        scratch_shapes=[
            pltpu.VMEM((chunks * PITCH, LANES), F32),
            pltpu.VMEM((2 * blocks, LANES), F32),
            pltpu.VMEM((channels, chunks + 16, width), F32),
            pltpu.VMEM((channels, chunks + 16, width), F32),
            pltpu.VMEM((channels * obs, frames), F32),
            pltpu.VMEM(fading.shape, F32),
            pltpu.VMEM(transition.shape, F32),
            pltpu.VMEM(obs_map.shape, F32),
            pltpu.VMEM(measured_weighting.shape, F32),
            pltpu.SemaphoreType.DMA((5,)),
        ],
        compiler_params=pltpu.CompilerParams(vmem_limit_bytes=24 << 20),
        name="before",
    )(
        *(
            pltpu.with_memory_space_constraint(a, pltpu.HBM)
            for a in (
                observations.reshape(channels * obs, frames), fading, transition, obs_map,
                measured_weighting,
            )
        )
    )
    fade, powers = kept[3], kept[4]
    second = [
        spec((channels, chunks, width), F32),
        spec((channels, chunks, width), F32),
        spec((channels, chunks, LANES), F32),
        spec((channels, 2 * width, 2 * width), BF16),
        spec((channels, 3 * width, 2 * width), BF16),
        spec((channels, 2 * width, 4 * obs), BF16),
        spec((channels, CHUNK // 2, chunks, 2 * width), F32),
        spec((channels, CHUNK // 2, chunks, 2 * obs), F32),
    ]
    made = pl.pallas_call(
        between,
        out_shape=second,
        in_specs=[vmem] * len(kept),
        out_specs=[vmem] * len(second),
        scratch_shapes=[
            pltpu.VMEM((channels, LANES + chunks, width), F32),
            pltpu.VMEM((channels, LANES + chunks, width), F32),
            pltpu.VMEM((2 * blocks, LANES), F32),
        ],
        compiler_params=pltpu.CompilerParams(vmem_limit_bytes=24 << 20),
        cost_estimate=pl.CostEstimate(
            flops=4_000_000_000, bytes_accessed=8_000_000, transcendentals=0
        ),
        name="between",
    )(*kept)
    sections = lax.axis_size("tm")
    arrived = [
        lax.ppermute(ends, "tm", [(i, (i + s) % sections) for i in range(sections)])
        for s in (1, 2, 3)
    ]
    group = lax.axis_size("chan")
    rows, nis = pl.pallas_call(
        after,
        out_shape=[
            pltpu.HBM((channels, CHUNK, chunks, width), F32),
            spec((group, 1, blocks), F32),
        ],
        in_specs=[vmem] * (6 + len(second)),
        out_specs=[pl.BlockSpec(memory_space=pltpu.HBM), vmem],
        scratch_shapes=[
            pltpu.VMEM((channels, chunks + 8, width), F32),
            pltpu.VMEM((channels, 2, chunks + 8, width), F32),
            pltpu.VMEM((channels, CHUNK, chunks, width), F32),
            pltpu.SemaphoreType.DMA((channels, CHUNK // 2)),
        ],
        compiler_params=pltpu.CompilerParams(vmem_limit_bytes=24 << 20),
        cost_estimate=pl.CostEstimate(
            flops=4_000_000_000, bytes_accessed=8_000_000, transcendentals=0
        ),
        name="after",
    )(*arrived, *made, powers, triples, obs_precision)
    everything = lax.all_to_all(nis, "chan", split_axis=0, concat_axis=0, tiled=True)
    states = pl.pallas_call(
        write,
        out_shape=jax.ShapeDtypeStruct((channels, width, frames), F32),
        in_specs=[pl.BlockSpec(memory_space=pltpu.HBM), vmem],
        out_specs=pl.BlockSpec(memory_space=pltpu.HBM),
        scratch_shapes=[
            pltpu.VMEM((channels, chunks // 64, CHUNK, 64, width), F32),
            pltpu.VMEM((channels, width, frames), F32),
            pltpu.SemaphoreType.DMA((channels, chunks // 64)),
            pltpu.SemaphoreType.DMA((channels, chunks // 64)),
        ],
        compiler_params=pltpu.CompilerParams(vmem_limit_bytes=16 << 20),
        cost_estimate=pl.CostEstimate(
            flops=4_000_000_000, bytes_accessed=8 * channels * width * frames, transcendentals=0
        ),
        name="write",
    )(pltpu.with_memory_space_constraint(rows, pltpu.HBM), fade)
    return states, jnp.sum(everything, axis=(0, 1))


def solution(mesh):
    in_specs = (
        P("chan", None, "tm"),
        P("chan", None, None),
        P("chan", None, None),
        P("chan", None),
        P("chan", None),
        P("chan", "tm"),
    )
    out_specs = (P("chan", None, "tm"), P("tm"))
    return jax.shard_map(
        per_device, mesh=mesh, in_specs=in_specs, out_specs=out_specs, check_vma=False
    )
```

```python
import jax
import jax.numpy as jnp
from jax import lax
from jax.experimental import pallas as pl
from jax.experimental.pallas import tpu as pltpu
from jax.sharding import PartitionSpec as P

LANES = 128
CHUNK = 16
PITCH = 17
BATCH = 128
F32 = jnp.float32
BF16 = jnp.bfloat16
HIGHEST = lax.Precision.HIGHEST


def dot(a, b):
    return jnp.dot(a, b, preferred_element_type=F32)


def exact_dot(a, b):
    return jnp.dot(a, b, preferred_element_type=F32, precision=HIGHEST)


def halves(x):
    high = x.astype(BF16)
    low = (x - high.astype(F32)).astype(BF16)
    return high, low


def packed(m):
    high, low = halves(m)
    return jnp.concatenate([high, low], axis=1)


def side_by_side(x):
    high, low = halves(x)
    return jnp.concatenate([high, low], axis=1)


def thirds(x):
    first = x.astype(BF16)
    rest = x - first.astype(F32)
    second = rest.astype(BF16)
    return first, second, (rest - second.astype(F32)).astype(BF16)


def squared(x):
    a, b, c = thirds(x)
    pair = jnp.concatenate([a, b], axis=1)
    out = dot(pair, jnp.concatenate([pair, pair], axis=0))
    rest = dot(jnp.concatenate([a, c], axis=1), jnp.concatenate([c, a], axis=0))
    return out[:, :LANES] + (out[:, LANES:] + rest)


def times(x, both):
    weights = jnp.concatenate([both, both], axis=0)
    out = dot(side_by_side(x), weights)
    width = out.shape[1] // 2
    return out[:, :width] + out[:, width:]


def times_rows(x, both):
    return folded(dot(stacked(x), both))


def stacked(x):
    high = x.astype(BF16).astype(F32)
    return jnp.concatenate([high, x - high], axis=0).astype(BF16)


def folded(out):
    rows = out.shape[0] // 2
    out = out[:rows] + out[rows:]
    return out[:, :LANES] + out[:, LANES:]


def before(
    y_hbm, f_hbm, t_hbm, h_hbm, w_hbm,
    ends_ref, sums_ref, phi_ref, pairs_ref, fade_ref, powers_ref, last_ref, closed_ref, double_ref,
    gain_ref, seen_ref, triple_ref,
    yt_ref, inv_ref, tree_ref, treef_ref, y_ref, f_ref, t_ref, h_ref, w_ref, in_sem,
):
    small = [
        pltpu.make_async_copy(source, target, in_sem.at[k])
        for k, (source, target) in enumerate(
            ((f_hbm, f_ref), (t_hbm, t_ref), (h_hbm, h_ref), (w_hbm, w_ref))
        )
    ]
    large = pltpu.make_async_copy(y_hbm, y_ref, in_sem.at[4])
    for copy in small:
        copy.start()
    large.start()
    for copy in small:
        copy.wait()
    frames = y_ref.shape[1]
    blocks = frames // LANES
    chunks = frames // CHUNK
    per_block = LANES // CHUNK
    obs = h_ref.shape[1]
    lane = lax.broadcasted_iota(jnp.int32, (1, LANES), 1)

    for b in range(blocks):
        fade_ref[2 * b : 2 * b + 2, :] = f_ref[:, b * LANES : (b + 1) * LANES]
    run = fade_ref[...]
    shift = 1
    while shift < CHUNK:
        run = jnp.where(lane % CHUNK >= shift, run * pltpu.roll(run, shift, 1), run)
        shift *= 2
    fade_ref[...] = run
    inv_ref[...] = 1.0 / run

    half_lane = lane < obs
    closed, gain, seen = [None, None], [None, None], [None, None]

    def first_step():
        for c in range(2):
            t, h = t_ref[c], h_ref[c]
            eye = lax.broadcasted_iota(jnp.int32, (obs, obs), 0) == lax.broadcasted_iota(
                jnp.int32, (obs, obs), 1
            )
            column = jnp.sum(jnp.where(eye, w_ref[c : c + 1, :], 0.0), axis=1, keepdims=True)
            gain[c] = column * h
            gain_ref[c] = gain[c]
            t1, t2, t3 = thirds(t)
            h1, h2, h3 = thirds(jnp.concatenate([h, h], axis=0))
            seen[c] = lax.dot_general(
                jnp.concatenate([t1, t1, t1, t2, t2, t3], axis=1),
                jnp.concatenate([h1, h2, h3, h1, h2, h1], axis=1),
                (((1,), (1,)), ((), ())),
                preferred_element_type=F32,
            )
            seen_ref[c] = seen[c][:, :obs]

    def second_step():
        for c in range(2):
            q1, q2, q3 = (v.astype(F32) for v in thirds(seen[c]))
            mixed = jnp.where(half_lane, q1, q3)
            g1, g2, g3 = thirds(gain[c])
            closed[c] = t_ref[c] - dot(
                jnp.concatenate([q1, q2, mixed], axis=1).astype(BF16),
                jnp.concatenate([g1, g2, g1, g2, g3, g1], axis=0),
            )
            closed_ref[c] = closed[c]

    power, stack = [None, None], [None, None]

    def third_step():
        for c in range(2):
            power[c] = squared(closed[c])
            double_ref[c] = power[c]
            gb = times(gain[c], packed(closed[c]))
            stack[c] = jnp.concatenate([gb, gain[c]] if c == 0 else [gain[c], gb], axis=0)

    levels = chunks.bit_length() - 1
    first_level = CHUNK.bit_length() - 1
    exponent = 1
    below = [None, None]

    def advance():
        nonlocal exponent
        for c in range(2):
            both = packed(power[c])
            if exponent < first_level:
                stack[c] = jnp.concatenate([times(stack[c], both), stack[c]], axis=0)
            else:
                level = exponent - first_level
                powers_ref[c, level] = both
                if level % 2:
                    triple_ref[c, level // 2] = packed(times(below[c], both))
                below[c] = power[c]
            if exponent - first_level == levels - 1:
                last_ref[c] = power[c]
            else:
                power[c] = squared(power[c])
        exponent += 1

    first_step()
    second_step()
    third_step()
    large.wait()
    steps = [advance] * (levels + first_level - 1)
    row = lax.broadcasted_iota(jnp.int32, (per_block, LANES), 0)
    wide = lax.broadcasted_iota(jnp.int32, (per_block, LANES), 1)
    last = wide == row * CHUNK + (CHUNK - 1)
    for b in range(blocks):
        y = y_ref[:, b * LANES : (b + 1) * LANES]
        top = y[:obs] * inv_ref[2 * b : 2 * b + 1, :]
        bottom = y[obs:] * inv_ref[2 * b + 1 : 2 * b + 2, :]
        turned = jnp.concatenate([top, bottom], axis=0).T
        for r in range(per_block):
            at = (b * per_block + r) * PITCH
            yt_ref[at : at + CHUNK, :] = turned[r * CHUNK : (r + 1) * CHUNK]
        for c in range(2):
            value = jnp.where(last, fade_ref[2 * b + c : 2 * b + c + 1, :], 0.0)
            total = jnp.sum(value, axis=1, keepdims=True)
            phi_ref[c, b * per_block : (b + 1) * per_block, :] = jnp.broadcast_to(
                total, (per_block, LANES)
            )
        if b % 3 == 1 and steps:
            steps.pop(0)()

    for step in steps:
        step()

    low_half = lane < obs
    total = [jnp.zeros((chunks, 2 * LANES), F32) for _ in range(2)]
    for p in range(CHUNK // 2):
        even = yt_ref[pl.ds(2 * p, chunks, stride=PITCH), :]
        odd = pltpu.roll(yt_ref[pl.ds(2 * p + 1, chunks, stride=PITCH), :], obs, 1)
        for c in range(2):
            value = jnp.where(low_half, even, odd) if c == 0 else jnp.where(low_half, odd, even)
            pairs_ref[c, p] = side_by_side(value)
            both = packed(stack[c][p * LANES : (p + 1) * LANES])
            total[c] = total[c] + dot(pairs_ref[c, p], jnp.concatenate([both, both], axis=0))
    for c in range(2):
        sums_ref[c] = phi_ref[c] * (total[c][:, :LANES] + total[c][:, LANES:])

    source, factors, base, at = sums_ref, phi_ref, 0, 0
    for level in range(levels // 2):
        count = chunks >> (2 * level + 2)
        rows = max(count, 8)
        for c in range(2):
            e = [source[c, pl.ds(base + k, rows, stride=4), :] for k in range(4)]
            f = [factors[c, pl.ds(base + k, rows, stride=4), :] for k in range(4)]
            f2 = f[3] * f[2]
            f1 = f2 * f[1]
            weights = jnp.concatenate(
                [powers_ref[c, 2 * level], powers_ref[c, 2 * level + 1], triple_ref[c, level]],
                axis=0,
            )
            moved = jnp.concatenate([e[2] * f[3], e[1] * f2, e[0] * f1], axis=1)
            state = e[3] + folded(dot(stacked(moved), weights))
            factor = f1 * f[0]
            if level == levels // 2 - 1:
                ends_ref[c : c + 1, :] = state[:1]
                ends_ref[2 + c : 3 + c, :] = factor[:1]
            else:
                tree_ref[c, at : at + count, :] = state[:count]
                treef_ref[c, at : at + count, :] = factor[:count]
        source, factors, base = tree_ref, treef_ref, at
        at += count


def between(
    sums_ref, phi_ref, pairs_ref, fade_ref, powers_ref, last_ref, closed_ref, double_ref, gain_ref,
    seen_ref,
    scan_ref, cum_ref, square_ref, section_ref, stepx_ref, stepe_ref, partx_ref, parte_ref,
    pad_ref, padf_ref, tmp_ref,
):
    chunks = sums_ref.shape[1]
    blocks = chunks * CHUNK // LANES
    per_block = LANES // CHUNK
    obs = gain_ref.shape[1]

    run = fade_ref[...]
    for r in range(per_block):
        moved = pltpu.roll(run, (LANES - r * CHUNK) % LANES, 1) if r else run
        tmp_ref[...] = moved * moved
        for c in range(2):
            square_ref[c, pl.ds(r, blocks, stride=per_block), :] = tmp_ref[
                pl.ds(c, blocks, stride=2), :
            ]

    weights = []
    for c in range(2):
        section = squared(last_ref[c])
        section_ref[c] = jnp.concatenate([packed(section), packed(squared(section))], axis=0)
        b1, b2, g, q = closed_ref[c], double_ref[c], gain_ref[c], seen_ref[c]
        gb, bq, gq = exact_dot(g, b1), exact_dot(b1, q), exact_dot(g, q)
        high, low = halves(jnp.concatenate([b1, b2], axis=1))
        stepx_ref[c] = jnp.concatenate([high, high, low], axis=0)
        both = packed(jnp.concatenate([q, bq], axis=1))
        stepe_ref[c] = jnp.concatenate([both, both], axis=0)
        none = jnp.zeros((obs, obs), F32)
        top = jnp.concatenate([g, gb, none, gq], axis=1)
        bottom = jnp.concatenate([jnp.zeros_like(g), g, none, none], axis=1)
        high, low = halves(jnp.concatenate([top, bottom] if c == 0 else [bottom, top], axis=0))
        weights.append(jnp.concatenate([high, high, low], axis=0))
        pad_ref[c, :LANES, :] = jnp.zeros((LANES, LANES), F32)
        padf_ref[c, :LANES, :] = jnp.ones((LANES, LANES), F32)

    levels = powers_ref.shape[1]
    state = [sums_ref[c] for c in range(2)]
    factor = [phi_ref[c] for c in range(2)]
    for p in range(max(levels, CHUNK // 2)):
        for c in range(2):
            if p < levels:
                reach = 1 << p
                pad_ref[c, LANES:, :] = state[c]
                padf_ref[c, LANES:, :] = factor[c]
                moved = pad_ref[c, pl.ds(LANES - reach, chunks), :]
                state[c] = state[c] + factor[c] * times(moved, powers_ref[c, p])
                factor[c] = factor[c] * padf_ref[c, pl.ds(LANES - reach, chunks), :]
            if p < CHUNK // 2:
                y = pairs_ref[c, p]
                out = dot(jnp.concatenate([y, y[:, :LANES]], axis=1), weights[c])
                observed = y[:, :LANES].astype(F32) + y[:, LANES:].astype(F32)
                if c == 1:
                    observed = pltpu.roll(observed, obs, 1)
                partx_ref[c, p] = out[:, : 2 * LANES]
                parte_ref[c, p] = observed - out[:, 2 * LANES :]
    for c in range(2):
        scan_ref[c] = state[c]
        cum_ref[c] = factor[c]


def after(
    one_ref, two_ref, three_ref, scan_ref, cum_ref, square_ref, section_ref, stepx_ref, stepe_ref,
    partx_ref, parte_ref, powers_ref, triple_ref, weight_ref,
    rows_ref, nis_ref,
    carry_ref, pad_ref, xt_ref, sem,
):
    chunks = scan_ref.shape[1]
    blocks = chunks * CHUNK // LANES
    per_block = LANES // CHUNK
    obs = weight_ref.shape[1]
    levels = powers_ref.shape[1]
    position = lax.axis_index("tm")
    some = [(position >= k).astype(F32) for k in (1, 2, 3)]

    wide = lambda v: jnp.broadcast_to(v, (8, LANES))
    arrived = (one_ref, two_ref, three_ref)
    s = [[wide(r[c : c + 1, :] * m) for r, m in zip(arrived, some)] for c in range(2)]
    f = [[wide(r[2 + c : 3 + c, :] * m) for r, m in zip(arrived, some)] for c in range(2)]
    entering = []
    for c in range(2):
        earlier = jnp.concatenate([f[c][0] * s[c][1], f[c][0] * f[c][1] * s[c][2]], axis=1)
        entering.append(s[c][0] + folded(dot(stacked(earlier), section_ref[c])))
    for c in range(2):
        carry_ref[c, :8, :] = entering[c]
        pad_ref[c, 0, :8, :] = jnp.zeros((8, LANES), F32)
        pad_ref[c, 1, :8, :] = jnp.ones((8, LANES), F32)
        pad_ref[c, 0, 8:, :] = scan_ref[c]
        pad_ref[c, 1, 8:, :] = cum_ref[c]
    for level in range(levels // 2):
        reach = 1 << (2 * level)
        rows = max(reach, 8)
        for c in range(2):
            few = stacked(carry_ref[c, :rows, :])
            weights = (powers_ref[c, 2 * level], powers_ref[c, 2 * level + 1], triple_ref[c, level])
            moved = [folded(dot(few, m)) for m in weights]
            for k in range(3):
                carry_ref[c, pl.ds((k + 1) * reach, rows), :] = moved[k]
    x = [
        pad_ref[c, 0, pl.ds(7, chunks), :]
        + pad_ref[c, 1, pl.ds(7, chunks), :] * carry_ref[c, :chunks, :]
        for c in range(2)
    ]

    first_half = lax.broadcasted_iota(jnp.int32, (1, LANES), 1) < obs
    score = [jnp.zeros((chunks, LANES), F32) for _ in range(2)]
    copies = []
    waiting = [None, None]

    def settle(c):
        p, seen = waiting[c]
        innovation = parte_ref[c, p] - (seen[:, :LANES] + seen[:, LANES:])
        w = weight_ref[c : c + 1, :]
        term = innovation * innovation * jnp.concatenate([w, w], axis=1)
        a, b = square_ref[c, :, 2 * p : 2 * p + 1], square_ref[c, :, 2 * p + 1 : 2 * p + 2]
        score[c] = score[c] + term * jnp.where(first_half, a, b)

    for p in range(CHUNK // 2):
        both = [side_by_side(x[c]) for c in range(2)]
        out = [
            dot(jnp.concatenate([both[c], both[c][:, :LANES]], axis=1), stepx_ref[c])
            for c in range(2)
        ]
        if p:
            for c in range(2):
                settle(c)
        for c in range(2):
            waiting[c] = p, dot(both[c], stepe_ref[c])
        for c in range(2):
            x[c] = partx_ref[c, p, :, LANES:] + out[c][:, LANES:]
            xt_ref[c, 2 * p] = partx_ref[c, p, :, :LANES] + out[c][:, :LANES]
            xt_ref[c, 2 * p + 1] = x[c]
            pair = pl.ds(2 * p, 2)
            copy = pltpu.make_async_copy(
                xt_ref.at[c, pair], rows_ref.at[c, pair], sem.at[c, p]
            )
            copy.start()
            copies.append(copy)
    for c in range(2):
        settle(c)

    total = score[0] + score[1]
    per_batch = jnp.sum(total.reshape(blocks, per_block, LANES), axis=1)
    local = lax.dot_general(
        jnp.ones((8, 3 * LANES), BF16), jnp.concatenate(thirds(per_batch), axis=1),
        (((1,), (1,)), ((), ())), preferred_element_type=F32,
    )
    divisor = 2 * nis_ref.shape[0] * BATCH * obs
    nis_ref[...] = jnp.broadcast_to((local[:1] / divisor)[None], nis_ref.shape)
    for copy in copies:
        copy.wait()


def write(rows_ref, fade_ref, out_ref, xt_ref, stage_ref, in_sem, out_sem):
    channels, steps, chunks, _ = rows_ref.shape
    per_block = LANES // CHUNK
    group = 64
    arriving = {}
    for k in range(chunks // group):
        for c in range(channels):
            part = pl.ds(k * group, group)
            arriving[k, c] = pltpu.make_async_copy(
                rows_ref.at[c, :, part], xt_ref.at[c, k], in_sem.at[c, k]
            )
            arriving[k, c].start()
    leaving = []
    for k in range(chunks // group):
        for c in range(channels):
            arriving[k, c].wait()
            flat = xt_ref.at[c, k]
            for b in range(group // per_block):
                tall = jnp.concatenate(
                    [flat[:, b * per_block + i, :] for i in range(per_block)], axis=0
                )
                block = k * (group // per_block) + b
                row = fade_ref[2 * block + c : 2 * block + c + 1, :]
                stage_ref[c, :, block * LANES : (block + 1) * LANES] = tall.T * row
            columns = pl.ds(k * group * CHUNK, group * CHUNK)
            copy = pltpu.make_async_copy(
                stage_ref.at[c, :, columns], out_ref.at[c, :, columns], out_sem.at[c, k]
            )
            copy.start()
            leaving.append(copy)
    for copy in leaving:
        copy.wait()


def per_device(observations, transition, obs_map, measured_weighting, obs_precision, fading):
    channels, obs, frames = observations.shape
    width = transition.shape[1]
    chunks = frames // CHUNK
    levels = chunks.bit_length() - 1
    blocks = frames // LANES
    vmem = pl.BlockSpec(memory_space=pltpu.VMEM)
    spec = jax.ShapeDtypeStruct
    first = [
        spec((2 * channels, width), F32),
        spec((channels, chunks, width), F32),
        spec((channels, chunks, width), F32),
        spec((channels, CHUNK // 2, chunks, 2 * LANES), BF16),
        spec((2 * blocks, LANES), F32),
        spec((channels, levels, width, 2 * width), BF16),
        spec((channels, width, width), F32),
        spec((channels, width, width), F32),
        spec((channels, width, width), F32),
        spec((channels, obs, width), F32),
        spec((channels, width, obs), F32),
        spec((channels, levels // 2, width, 2 * width), BF16),
    ]
    ends, *kept, triples = pl.pallas_call(
        before,
        out_shape=first,
        in_specs=[pl.BlockSpec(memory_space=pltpu.HBM)] * 5,
        out_specs=[vmem] * len(first),
        scratch_shapes=[
            pltpu.VMEM((chunks * PITCH, LANES), F32),
            pltpu.VMEM((2 * blocks, LANES), F32),
            pltpu.VMEM((channels, chunks + 16, width), F32),
            pltpu.VMEM((channels, chunks + 16, width), F32),
            pltpu.VMEM((channels * obs, frames), F32),
            pltpu.VMEM(fading.shape, F32),
            pltpu.VMEM(transition.shape, F32),
            pltpu.VMEM(obs_map.shape, F32),
            pltpu.VMEM(measured_weighting.shape, F32),
            pltpu.SemaphoreType.DMA((5,)),
        ],
        compiler_params=pltpu.CompilerParams(vmem_limit_bytes=24 << 20),
        name="before",
    )(
        *(
            pltpu.with_memory_space_constraint(a, pltpu.HBM)
            for a in (
                observations.reshape(channels * obs, frames), fading, transition, obs_map,
                measured_weighting,
            )
        )
    )
    fade, powers = kept[3], kept[4]
    second = [
        spec((channels, chunks, width), F32),
        spec((channels, chunks, width), F32),
        spec((channels, chunks, LANES), F32),
        spec((channels, 2 * width, 2 * width), BF16),
        spec((channels, 3 * width, 2 * width), BF16),
        spec((channels, 2 * width, 4 * obs), BF16),
        spec((channels, CHUNK // 2, chunks, 2 * width), F32),
        spec((channels, CHUNK // 2, chunks, 2 * obs), F32),
    ]
    made = pl.pallas_call(
        between,
        out_shape=second,
        in_specs=[vmem] * len(kept),
        out_specs=[vmem] * len(second),
        scratch_shapes=[
            pltpu.VMEM((channels, LANES + chunks, width), F32),
            pltpu.VMEM((channels, LANES + chunks, width), F32),
            pltpu.VMEM((2 * blocks, LANES), F32),
        ],
        compiler_params=pltpu.CompilerParams(vmem_limit_bytes=24 << 20),
        cost_estimate=pl.CostEstimate(
            flops=4_000_000_000, bytes_accessed=8_000_000, transcendentals=0
        ),
        name="between",
    )(*kept)
    sections = lax.axis_size("tm")
    arrived = [
        lax.ppermute(ends, "tm", [(i, (i + s) % sections) for i in range(sections)])
        for s in (1, 2, 3)
    ]
    group = lax.axis_size("chan")
    rows, nis = pl.pallas_call(
        after,
        out_shape=[
            pltpu.HBM((channels, CHUNK, chunks, width), F32),
            spec((group, 1, blocks), F32),
        ],
        in_specs=[vmem] * (6 + len(second)),
        out_specs=[pl.BlockSpec(memory_space=pltpu.HBM), vmem],
        scratch_shapes=[
            pltpu.VMEM((channels, chunks + 8, width), F32),
            pltpu.VMEM((channels, 2, chunks + 8, width), F32),
            pltpu.VMEM((channels, CHUNK, chunks, width), F32),
            pltpu.SemaphoreType.DMA((channels, CHUNK // 2)),
        ],
        compiler_params=pltpu.CompilerParams(vmem_limit_bytes=24 << 20),
        cost_estimate=pl.CostEstimate(
            flops=4_000_000_000, bytes_accessed=8_000_000, transcendentals=0
        ),
        name="after",
    )(*arrived, *made, powers, triples, obs_precision)
    everything = lax.all_to_all(nis, "chan", split_axis=0, concat_axis=0, tiled=True)
    states = pl.pallas_call(
        write,
        out_shape=jax.ShapeDtypeStruct((channels, width, frames), F32),
        in_specs=[pl.BlockSpec(memory_space=pltpu.HBM), vmem],
        out_specs=pl.BlockSpec(memory_space=pltpu.HBM),
        scratch_shapes=[
            pltpu.VMEM((channels, chunks // 64, CHUNK, 64, width), F32),
            pltpu.VMEM((channels, width, frames), F32),
            pltpu.SemaphoreType.DMA((channels, chunks // 64)),
            pltpu.SemaphoreType.DMA((channels, chunks // 64)),
        ],
        compiler_params=pltpu.CompilerParams(vmem_limit_bytes=16 << 20),
        cost_estimate=pl.CostEstimate(
            flops=4_000_000_000, bytes_accessed=8 * channels * width * frames, transcendentals=0
        ),
        name="write",
    )(pltpu.with_memory_space_constraint(rows, pltpu.HBM), fade)
    return states, jnp.sum(everything, axis=(0, 1))


def solution(mesh):
    in_specs = (
        P("chan", None, "tm"),
        P("chan", None, None),
        P("chan", None, None),
        P("chan", None),
        P("chan", None),
        P("chan", "tm"),
    )
    out_specs = (P("chan", None, "tm"), P("tm"))
    return jax.shard_map(
        per_device, mesh=mesh, in_specs=in_specs, out_specs=out_specs, check_vma=False
    )
```
